32 devices in a mesh: loc: 8 (over y, x, core), stream: 4 (over z).
Axes of the slice: x: 2, y: 2, z: 4, core: 2. Of those that a mesh axis runs over, the one named last changes fastest.
Arguments:
- latent: bfloat16 [12288, 1024], P(('loc', 'stream')), may hold values from -7 to 7
- observations: bfloat16 [4, 8, 8, 32, 1024], P('stream', 'loc'), may hold values from -7 to 7
- counts: int32 [4, 8, 8], P('stream', 'loc'), may hold values from 1 to 32, as said below
- cross_query: bfloat16 [1024, 1024], replicated, may hold values from -1 to 1
- cross_kv: bfloat16 [1024, 2048], replicated, may hold values from -1 to 1
- cross_out: bfloat16 [1024, 1024], replicated, may hold values from -0.1875 to 0.1875
- self_qkv: bfloat16 [1024, 3072], replicated, may hold values from -1 to 1
- self_out: bfloat16 [1024, 1024], replicated, may hold values from -0.1875 to 0.1875
- mlp_in: bfloat16 [1024, 4096], P(None, ('loc', 'stream')), may hold values from -0.1875 to 0.1875
- mlp_out: bfloat16 [1024, 4096], P(None, ('loc', 'stream')), may hold values from -0.09375 to 0.09375
Outputs:
- forecast: bfloat16 [12288, 1024], P(('loc', 'stream'))
The draws below stay inside these ranges and needn't reach their ends.
Inputs may be any that keep to these rules, and one draw needn't show every extreme that they name: `counts`: slots 0 to count - 1 of a block hold observations and the rest are padding; for every stream some section receives 32 rows from every ingest shard.
All inputs are finite; a program needn't handle non-finite values.
Results may differ from the reference program's by a relative error of at most 0.013.
Values may be sent and summed in bfloat16 or wider, within the bound.
No kernel may reach another device: no remote copies, remote signals or barrier semaphores. Data moves between devices by JAX's collectives and lax.ppermute only.
A program may use at most 192 MiB of HBM per device.

```python
import math
import jax
import jax.numpy as jnp
from jax import lax

D = 1024
HEADS = 16
FF = 4096
WIN = 512
NODE_DEV = 384
CAP = 32
NODES = 12288
N_LOC = 8
N_STREAM = 4


def base_weight(key, fold_value, array_shape):
    noise_draw = jax.random.normal(jax.random.fold_in(key, fold_value), array_shape, jnp.float32)
    return jnp.clip(noise_draw, -6.0, 6.0) / math.sqrt(array_shape[0])


def feature_rows(key, fold_value, array_shape):
    noise_draw = jax.random.normal(jax.random.fold_in(key, fold_value), array_shape, jnp.float32)
    return jnp.clip(noise_draw, -6.0, 6.0)


def draw_latent(key, part):
    return feature_rows(key, 701, (NODES, D)).astype(jnp.bfloat16)


def draw_observations(key, part):
    return feature_rows(key, 711, (N_STREAM, N_LOC, N_LOC, CAP, D)).astype(jnp.bfloat16)


def draw_cross_query(key, part):
    weights = base_weight(key, 721, (D, D))
    return weights.astype(jnp.bfloat16)


def draw_cross_kv(key, part):
    weights = base_weight(key, 722, (D, 2 * D))
    return weights.astype(jnp.bfloat16)


def draw_self_qkv(key, part):
    weights = base_weight(key, 723, (D, 3 * D))
    return weights.astype(jnp.bfloat16)


def draw_counts(key, part):
    base_key = jax.random.fold_in(key, 11)
    load_key, fill_key, full_key = jax.random.split(base_key, 3)
    section_load = jax.random.randint(load_key, (N_STREAM, 1, N_LOC), 1, 5)
    raw_fill = jax.random.randint(fill_key, (N_STREAM, N_LOC, N_LOC), 0, CAP)
    filled = 1 + raw_fill * section_load // 4
    full_section = jax.random.randint(full_key, (N_STREAM, 1, 1), 0, N_LOC)
    section_index = lax.broadcasted_iota(jnp.int32, (N_STREAM, N_LOC, N_LOC), 2)
    filled = jnp.where(section_index == full_section, CAP, filled)
    return filled.astype(jnp.int32)


def levels(stream_key, shape, cuts, low, high):
    gain, own = 1.0, jax.random.fold_in(stream_key, 6)
    for axis_at, shards_of in cuts:
        draws = jnp.exp(jax.random.uniform(jax.random.fold_in(own, axis_at), (shards_of,), jnp.float32, low / len(cuts), high / len(cuts)))
        gain = gain * jnp.repeat(draws, shape[axis_at] // shards_of).reshape([-1 if axis == axis_at else 1 for axis in range(len(shape))])
    return gain


def noise(own_key, dims, width, limit, cuts=(), kind=jnp.bfloat16):
    values = jax.random.normal(own_key, dims, jnp.float32) * width
    if len(cuts) > 0:
        values = levels(own_key, dims, cuts, -0.22, 0.18) * values
    return jnp.clip(values, min=-limit, max=limit).astype(kind)


def setup_inputs(seed: int = 0) -> dict:
    key_of = jax.random.split(jax.random.key(seed), 11)
    return {
        "latent": draw_latent(jax.random.fold_in(key_of[10], 71), 0),
        "observations": draw_observations(jax.random.fold_in(key_of[10], 71), 0),
        "counts": draw_counts(jax.random.fold_in(key_of[10], 71), 0),
        "cross_query": draw_cross_query(jax.random.fold_in(key_of[10], 71), 0),
        "cross_kv": draw_cross_kv(jax.random.fold_in(key_of[10], 71), 0),
        "cross_out": noise(key_of[5], (D, D), D ** -0.5, 0.1875),
        "self_qkv": draw_self_qkv(jax.random.fold_in(key_of[10], 71), 0),
        "self_out": noise(key_of[7], (D, D), D ** -0.5, 0.1875),
        "mlp_in": noise(key_of[8], (D, FF), D ** -0.5, 0.1875, ((1, 32),)),
        "mlp_out": noise(key_of[9], (D, FF), FF ** -0.5, 0.09375, ((1, 32),)),
    }


EPSILON = 1e-06
MASKED = -1e+30

def rms_norm(tensor):
    floats = tensor.astype(jnp.float32)
    return (floats * lax.rsqrt(lax.optimization_barrier(jnp.mean(floats * floats, axis=-1, keepdims=True)) + EPSILON)).astype(jnp.bfloat16)

def masked_attention(queries, key_rows, value_rows, allowed):
    row_count = queries.shape[0]
    feat_width = queries.shape[1]
    head_width = feat_width // HEADS
    query_per_head = queries.astype(jnp.float32).reshape(row_count, HEADS, head_width)
    key_per_head = key_rows.astype(jnp.float32).reshape(key_rows.shape[0], HEADS, head_width)
    value_per_head = value_rows.astype(jnp.float32).reshape(value_rows.shape[0], HEADS, head_width)
    score_matrix = jnp.einsum('jsv,esv->sje', query_per_head, key_per_head) * (1.0 / math.sqrt(head_width))
    score_matrix = jnp.where(allowed[None], score_matrix, MASKED)
    row_max = lax.optimization_barrier(jnp.max(score_matrix, axis=2, keepdims=True))
    exp_terms = jnp.where(allowed[None], jnp.exp(score_matrix - row_max), 0.0)
    row_sum = lax.optimization_barrier(jnp.sum(exp_terms, axis=2))
    rounded_values = lax.optimization_barrier(exp_terms.astype(jnp.bfloat16))
    mixed_output = jnp.einsum('lsu,uly->sly', rounded_values.astype(jnp.float32), value_per_head)
    mixed_output = mixed_output / jnp.transpose(row_sum)[:, :, None]
    return mixed_output.reshape(row_count, feat_width).astype(jnp.bfloat16)

def reference(latent, observations, counts, cross_query, cross_kv, cross_out, self_qkv, self_out, mlp_in, mlp_out):
    feat_width = latent.shape[1]
    slot_index = lax.broadcasted_iota(jnp.int32, observations.shape[:4], 3)
    live = slot_index < counts[..., None]
    obs_kv = jnp.dot(rms_norm(observations.reshape(-1, feat_width)), cross_kv, preferred_element_type=jnp.float32).astype(jnp.bfloat16)
    obs_kv = obs_kv.reshape(N_STREAM, N_LOC, N_LOC, CAP, 2 * feat_width)
    queries = jnp.dot(rms_norm(latent), cross_query, preferred_element_type=jnp.float32).astype(jnp.bfloat16)
    block_total = N_LOC * N_STREAM

    def cross_block(block_index):
        section = block_index // N_STREAM
        section_kv = lax.dynamic_index_in_dim(obs_kv, section, 2, keepdims=False).reshape(-1, 2 * feat_width)
        section_live = lax.dynamic_index_in_dim(live, section, 2, keepdims=False).reshape(-1)
        block_rows = lax.dynamic_slice_in_dim(queries, (block_index * NODE_DEV).astype(jnp.int32), NODE_DEV, 0)
        allowed = jnp.broadcast_to(section_live[None, :], (NODE_DEV, section_live.shape[0]))
        return masked_attention(block_rows, section_kv[:, :feat_width], section_kv[:, feat_width:], allowed)
    cross_ctx = lax.map(cross_block, jnp.arange(block_total, dtype=jnp.int32)).reshape(-1, feat_width)
    after_cross = (latent.astype(jnp.float32) + jnp.dot(cross_ctx, cross_out, preferred_element_type=jnp.float32)).astype(jnp.bfloat16)
    self_proj = jnp.dot(rms_norm(after_cross), self_qkv, preferred_element_type=jnp.float32).astype(jnp.bfloat16)
    half_win = WIN // 2
    padded_kv = jnp.pad(self_proj[:, feat_width:], ((half_win, half_win), (0, 0)))

    def window_block(block_index):
        offset = (block_index * NODE_DEV).astype(jnp.int32)
        block_rows = lax.dynamic_slice_in_dim(self_proj[:, :feat_width], offset, NODE_DEV, 0)
        window_kv = lax.dynamic_slice_in_dim(padded_kv, offset, NODE_DEV + 2 * half_win, 0)
        query_pos = offset + lax.broadcasted_iota(jnp.int32, (NODE_DEV, 1), 0)
        key_pos = offset - half_win + lax.broadcasted_iota(jnp.int32, (1, NODE_DEV + 2 * half_win), 1)
        allowed = (jnp.abs(query_pos - key_pos) <= half_win) & (key_pos >= 0) & (key_pos < NODES)
        self_ctx = masked_attention(block_rows, window_kv[:, :feat_width], window_kv[:, feat_width:], allowed)
        residual = lax.dynamic_slice_in_dim(after_cross, offset, NODE_DEV, 0)
        after_self = (residual.astype(jnp.float32) + jnp.dot(self_ctx, self_out, preferred_element_type=jnp.float32)).astype(jnp.bfloat16)
        hidden = jax.nn.gelu(jnp.dot(rms_norm(after_self), mlp_in, preferred_element_type=jnp.float32), approximate=True).astype(jnp.bfloat16)
        grown = jnp.dot(hidden, jnp.transpose(mlp_out), preferred_element_type=jnp.float32)
        return (after_self.astype(jnp.float32) + grown).astype(jnp.bfloat16)
    return lax.map(window_block, jnp.arange(block_total, dtype=jnp.int32)).reshape(-1, feat_width)
```

```python
import functools
import math

import jax
import jax.numpy as jnp
from jax import lax
from jax.experimental import pallas as pl
from jax.experimental.pallas import tpu as pltpu
from jax.sharding import PartitionSpec as P

HEADS = 16
WIN = 512

EPSILON = 1e-06
MASKED = -1e30
LANES = 128
ROWS = 128
SCORES = 1 << 19


F32 = jnp.float32
BF16 = jnp.bfloat16


def rms_norm(tensor):
    floats = tensor.astype(F32)
    return (floats * lax.rsqrt(jnp.mean(floats * floats, axis=-1, keepdims=True) + EPSILON)).astype(BF16)


def dot(a, b):
    return jnp.dot(a, b, preferred_element_type=F32)


def dot_t(a, b):
    return lax.dot_general(a, b, (((1,), (1,)), ((), ())), preferred_element_type=F32)


def vmem():
    return pl.BlockSpec(memory_space=pltpu.VMEM)


def params(mib):
    return pltpu.CompilerParams(vmem_limit_bytes=mib << 20)


def head_sides(width):
    lane = lax.broadcasted_iota(jnp.int32, (1, LANES), 1)
    return [(lane >= at) & (lane < at + width) for at in range(0, LANES, width)]


def softmax_part(query, keys, values, sides, bias=None, masks=()):
    peak = mixed = total = None
    for side in sides:
        if bias is None:
            score = dot_t(query, jnp.where(side, keys, jnp.zeros_like(keys)))
        else:
            score = dot_t(jnp.where(side, query, jnp.ones_like(query)), jnp.where(side, keys, bias))
        if masks:
            blocks = [score[:, at : at + ROWS] for at in range(0, score.shape[1], ROWS)]
            for index, mask in masks:
                blocks[index] = blocks[index] + mask
            score = jnp.concatenate(blocks, axis=1)
        top = jnp.max(score, axis=1, keepdims=True)
        weight = jnp.exp(score - top).astype(BF16)
        both = dot(weight, jnp.where(side, values, jnp.ones_like(values)))
        other = pltpu.roll(both, LANES // len(sides), 1)
        top = jnp.broadcast_to(top, both.shape)
        if peak is None:
            peak, mixed, total = top, both, other
        else:
            peak, mixed, total = (
                jnp.where(side, new, old) for new, old in ((top, peak), (both, mixed), (other, total))
            )
    return peak, mixed, total


def merge(first, second):
    peak = jnp.maximum(first[0], second[0])
    left, right = jnp.exp(first[0] - peak), jnp.exp(second[0] - peak)
    mixed = first[1] * left + second[1] * right
    total = first[2] * left + second[2] * right
    return mixed / total


def tile_at(tile):
    return pl.ds(pl.multiple_of(tile * LANES, LANES), LANES)


def row_step(nodes, keys):
    return nodes if nodes * keys <= SCORES else math.gcd(nodes, ROWS)


def project_observations(chunks, w_kv, keys, values, bias):
    feat = w_kv.shape[0]
    base = 0
    for chunk in chunks:
        size = chunk.shape[0]
        block = chunk[...].astype(F32)
        live = block[:, :1] < jnp.inf
        normed = rms_norm(jnp.where(live, block, 0.0))
        part = slice(base, base + size)
        keys[part] = dot(normed, w_kv[:, :feat]).astype(BF16)
        values[part] = dot(normed, w_kv[:, feat:]).astype(BF16)
        bias[part] = jnp.broadcast_to(jnp.where(live, 0.0, MASKED), (size, LANES)).astype(BF16)
        base += size


def cross_head_kernel(width, query, w_kv, *refs):
    chunks, (peak, mixed, total, keys, values, bias) = refs[:-6], refs[-6:]
    nodes, feat = query.shape
    project_observations(chunks, w_kv, keys, values, bias)
    sides = head_sides(width)
    step = row_step(nodes, keys.shape[0])

    @pl.loop(0, feat // LANES)
    def _(tile):
        at = tile_at(tile)
        for start in range(0, nodes, step):
            part = slice(start, start + step)
            peak[part, at], mixed[part, at], total[part, at] = softmax_part(
                query[part, at], keys[:, at], values[:, at], sides, bias[...]
            )


def cross_tail_kernel(width, latent, query, w_kv, w_out, peak, mixed, total, chunk, out, keys, values, bias, ctx):
    nodes, feat = query.shape
    project_observations([chunk], w_kv, keys, values, bias)
    sides = head_sides(width)
    step = row_step(nodes, keys.shape[0])

    @pl.loop(0, feat // LANES)
    def _(tile):
        at = tile_at(tile)
        for start in range(0, nodes, step):
            part = slice(start, start + step)
            last = softmax_part(query[part, at], keys[:, at], values[:, at], sides, bias[...])
            ctx[part, at] = merge((peak[part, at], mixed[part, at], total[part, at]), last).astype(BF16)

    out[...] = (latent[...].astype(F32) + dot(ctx[...], w_out[...])).astype(BF16)


def cross_attention(latent, queries, rows, w_kv, w_out):
    nodes, feat = latent.shape
    width = feat // HEADS
    chunks, last = rows[:-1], rows[-1]
    size = sum(chunk.shape[0] for chunk in chunks)
    state = pl.pallas_call(
        functools.partial(cross_head_kernel, width),
        out_shape=[jax.ShapeDtypeStruct((nodes, feat), F32)] * 3,
        in_specs=[vmem()] * (2 + len(chunks)),
        out_specs=[vmem()] * 3,
        scratch_shapes=[
            pltpu.VMEM((size, feat), BF16),
            pltpu.VMEM((size, feat), BF16),
            pltpu.VMEM((size, LANES), BF16),
        ],
        compiler_params=params(56),
        cost_estimate=pl.CostEstimate(flops=16_000_000_000, bytes_accessed=12 << 20, transcendentals=0),
        name="cross_head",
    )(queries, w_kv, *chunks)
    size = last.shape[0]
    return pl.pallas_call(
        functools.partial(cross_tail_kernel, width),
        out_shape=jax.ShapeDtypeStruct((nodes, feat), BF16),
        in_specs=[vmem()] * 8,
        out_specs=vmem(),
        scratch_shapes=[
            pltpu.VMEM((size, feat), BF16),
            pltpu.VMEM((size, feat), BF16),
            pltpu.VMEM((size, LANES), BF16),
            pltpu.VMEM((nodes, feat), BF16),
        ],
        compiler_params=params(40),
        cost_estimate=pl.CostEstimate(flops=7_000_000_000, bytes_accessed=12 << 20, transcendentals=0),
        name="cross_tail",
    )(latent, queries, w_kv, w_out, *state, last)


def edge_masks():
    row = lax.broadcasted_iota(jnp.int32, (ROWS, ROWS), 0)
    col = lax.broadcasted_iota(jnp.int32, (ROWS, ROWS), 1)
    return jnp.where(col >= row, 0.0, MASKED), jnp.where(col <= row, 0.0, MASKED)


def window_local_kernel(width, half, own, w_qkv, query, peak, mixed, total, keys, values):
    nodes, feat = own.shape
    normed = rms_norm(own[...])
    scale = jnp.asarray(1.0 / math.sqrt(width), BF16)
    query[...] = dot(normed, w_qkv[:, :feat]).astype(BF16) * scale
    keys[...] = dot(normed, w_qkv[:, feat : 2 * feat]).astype(BF16)
    values[...] = dot(normed, w_qkv[:, 2 * feat :]).astype(BF16)
    sides = head_sides(width)
    reach = half // ROWS
    count = nodes // ROWS
    before, after = edge_masks()

    @pl.loop(0, feat // LANES)
    def _(tile):
        at = tile_at(tile)
        for block in range(count):
            part = slice(block * ROWS, (block + 1) * ROWS)
            low, high = max(0, block - reach), min(count, block + reach + 1)
            masks = []
            if block - reach >= 0:
                masks.append((0, before))
            if block + reach < count:
                masks.append((high - low - 1, after))
            span = slice(low * ROWS, high * ROWS)
            peak[part, at], mixed[part, at], total[part, at] = softmax_part(
                query[part, at], keys[span, at], values[span, at], sides, masks=masks
            )


def window_halo_kernel(
    width, edge, own, query, peak, mixed, total, low, high, w_qkv, w_out, out, keys, values, bias, ctx
):
    nodes, feat = own.shape
    half = low.shape[0]
    for base, rows, gate in ((0, low, 0), (half, high, 1)):
        normed = rms_norm(rows[...])
        part = slice(base, base + half)
        keys[part] = dot(normed, w_qkv[:, feat : 2 * feat]).astype(BF16)
        values[part] = dot(normed, w_qkv[:, 2 * feat :]).astype(BF16)
        bias[part] = jnp.full((half, LANES), edge[gate], F32).astype(BF16)
    sides = head_sides(width)
    reach = half // ROWS
    count = nodes // ROWS
    before, after = edge_masks()

    @pl.loop(0, feat // LANES)
    def _(tile):
        at = tile_at(tile)
        for block in range(count):
            part = slice(block * ROWS, (block + 1) * ROWS)
            first, stop = min(block, reach), max(reach, block + 2 * reach - count + 1)
            state = (peak[part, at], mixed[part, at], total[part, at])
            if stop > first:
                masks = []
                if block < reach:
                    masks.append((0, before))
                if block + 2 * reach - count >= reach:
                    masks.append((stop - first - 1, after))
                span = slice(first * ROWS, stop * ROWS)
                other = softmax_part(query[part, at], keys[span, at], values[span, at], sides, bias[span], masks)
                ctx[part, at] = merge(state, other).astype(BF16)
            else:
                ctx[part, at] = (state[1] / state[2]).astype(BF16)

    out[...] = (own[...].astype(F32) + dot(ctx[...], w_out[...])).astype(BF16)


def window_local(own, half, w_qkv):
    nodes, feat = own.shape
    return pl.pallas_call(
        functools.partial(window_local_kernel, feat // HEADS, half),
        out_shape=[jax.ShapeDtypeStruct((nodes, feat), BF16)] + [jax.ShapeDtypeStruct((nodes, feat), F32)] * 3,
        in_specs=[vmem()] * 2,
        out_specs=[vmem()] * 4,
        scratch_shapes=[pltpu.VMEM((nodes, feat), BF16), pltpu.VMEM((nodes, feat), BF16)],
        compiler_params=params(40),
        cost_estimate=pl.CostEstimate(flops=15_000_000_000, bytes_accessed=12 << 20, transcendentals=0),
        name="window_local",
    )(own, w_qkv)


def window_halo(edge, own, local, low, high, w_qkv, w_out):
    nodes, feat = own.shape
    half = low.shape[0]
    return pl.pallas_call(
        functools.partial(window_halo_kernel, feat // HEADS),
        out_shape=jax.ShapeDtypeStruct((nodes, feat), BF16),
        in_specs=[pl.BlockSpec(memory_space=pltpu.SMEM)] + [vmem()] * 9,
        out_specs=vmem(),
        scratch_shapes=[
            pltpu.VMEM((2 * half, feat), BF16),
            pltpu.VMEM((2 * half, feat), BF16),
            pltpu.VMEM((2 * half, LANES), BF16),
            pltpu.VMEM((nodes, feat), BF16),
        ],
        compiler_params=params(40),
        cost_estimate=pl.CostEstimate(flops=10_000_000_000, bytes_accessed=12 << 20, transcendentals=0),
        name="window_halo",
    )(edge, own, *local, low, high, w_qkv, w_out)


def mlp_kernel(group, rows, *refs):
    pieces, (out, held, normed, total, sems) = refs[:-5], refs[-5:]
    slots = held.shape[0]
    blocks = [(piece, at) for piece in pieces for at in range(0, piece.shape[0], group)]

    def copy(index):
        piece, at = blocks[index]
        slot = index % slots
        return pltpu.make_async_copy(piece.at[pl.ds(at, group)], held.at[slot], sems.at[slot])

    for index in range(min(slots - 1, len(blocks))):
        copy(index).start()
    normed[...] = rms_norm(rows[...])
    total[...] = rows[...].astype(F32)
    for index in range(len(blocks)):
        if index + slots - 1 < len(blocks):
            copy(index + slots - 1).start()
        copy(index).wait()
        slot = index % slots
        w_in = jnp.concatenate([held[slot, k, 0] for k in range(group)], axis=1)
        w_back = jnp.concatenate([held[slot, k, 1] for k in range(group)], axis=1)
        hidden = jax.nn.gelu(dot(normed[...], w_in), approximate=True).astype(BF16)
        total[...] += dot_t(hidden, w_back)
    out[...] = total[...].astype(BF16)


def mlp(rows, pieces):
    nodes, feat = rows.shape
    shards, _, _, width = pieces[0].shape
    group = math.gcd(shards, max(1, 512 // width))
    return pl.pallas_call(
        functools.partial(mlp_kernel, group),
        out_shape=jax.ShapeDtypeStruct((nodes, feat), BF16),
        in_specs=[vmem()] + [pl.BlockSpec(memory_space=pl.ANY)] * len(pieces),
        out_specs=vmem(),
        scratch_shapes=[
            pltpu.VMEM((3, group, 2, feat, width), BF16),
            pltpu.VMEM((nodes, feat), BF16),
            pltpu.VMEM((nodes, feat), F32),
            pltpu.SemaphoreType.DMA((3,)),
        ],
        compiler_params=params(60),
        cost_estimate=pl.CostEstimate(flops=8_000_000_000, bytes_accessed=18 << 20, transcendentals=0),
        name="mlp",
    )(rows, *pieces)


def shards(
    latent,
    observations,
    counts,
    cross_query,
    cross_kv,
    cross_out,
    self_qkv,
    self_out,
    mlp_in,
    mlp_out,
):
    everyone = ("loc", "stream")
    feat = latent.shape[1]
    width = feat // HEADS
    half = WIN // 2
    streams = lax.axis_size("stream")
    def rotate(value, shift):
        return lax.ppermute(value, "stream", [(i, (i + shift) % streams) for i in range(streams)])

    shifts = sorted(range(1, streams), key=lambda shift: min(shift, streams - shift))
    near, far = shifts[:-1], shifts[-1:]
    held = jnp.stack([mlp_in, mlp_out])[None]
    pieces = [lax.all_gather(held, everyone, axis=0, tiled=True)]
    slot = lax.broadcasted_iota(jnp.int32, observations.shape[:4], 3)
    marked = jnp.where((slot < counts[..., None])[..., None], observations, jnp.asarray(jnp.inf, BF16))
    moved = lax.all_to_all(marked, "loc", split_axis=2, concat_axis=1, tiled=True).reshape(-1, feat)
    rows = [moved] + [rotate(moved, shift) for shift in near + far]
    queries = dot(rms_norm(latent), cross_query).astype(BF16) * jnp.asarray(1.0 / math.sqrt(width), BF16)
    after_cross = cross_attention(latent, queries, rows, cross_kv, cross_out)
    count = lax.axis_size(everyone)
    low = lax.ppermute(after_cross[-half:], everyone, [(i, i + 1) for i in range(count - 1)])
    high = lax.ppermute(after_cross[:half], everyone, [(i + 1, i) for i in range(count - 1)])
    local = window_local(after_cross, half, self_qkv)
    place = lax.axis_index(everyone)
    edge = jnp.where(jnp.stack([place == 0, place == count - 1]), MASKED, 0.0).astype(F32)
    after_self = window_halo(edge, after_cross, local, low, high, self_qkv, self_out)
    return mlp(after_self, pieces)


def solution(mesh):
    return jax.shard_map(
        shards,
        mesh=mesh,
        in_specs=(
            P(("loc", "stream"), None),
            P("stream", "loc", None, None, None),
            P("stream", "loc", None),
            P(),
            P(),
            P(),
            P(),
            P(),
            P(None, ("loc", "stream")),
            P(None, ("loc", "stream")),
        ),
        out_specs=P(("loc", "stream"), None),
        check_vma=False,
    )
```

```python
import functools
import math

import jax
import jax.numpy as jnp
from jax import lax
from jax.experimental import pallas as pl
from jax.experimental.pallas import tpu as pltpu
from jax.sharding import PartitionSpec as P


HEADS = 16
WIN = 512

EPSILON = 1e-06
MASKED = -1e30
LANES = 128
ROWS = 128
SCORES = 1 << 19


F32 = jnp.float32
BF16 = jnp.bfloat16


def rms_norm(tensor):
    floats = tensor.astype(F32)
    return (floats * lax.rsqrt(jnp.mean(floats * floats, axis=-1, keepdims=True) + EPSILON)).astype(BF16)


def dot(a, b):
    return jnp.dot(a, b, preferred_element_type=F32)


def dot_t(a, b):
    return lax.dot_general(a, b, (((1,), (1,)), ((), ())), preferred_element_type=F32)


def vmem():
    return pl.BlockSpec(memory_space=pltpu.VMEM)


def hbm():
    return pl.BlockSpec(memory_space=pltpu.HBM)


def params(mib):
    return pltpu.CompilerParams(vmem_limit_bytes=mib << 20)


def head_sides(width):
    lane = lax.broadcasted_iota(jnp.int32, (1, LANES), 1)
    return [(lane >= at) & (lane < at + width) for at in range(0, LANES, width)]


def softmax_part(query, keys, values, sides, bias=None, masks=None):
    peak = mixed = total = None
    for side in sides:
        if bias is None:
            score = dot_t(query, jnp.where(side, keys, jnp.zeros_like(keys)))
        else:
            score = dot_t(jnp.where(side, query, jnp.ones_like(query)), jnp.where(side, keys, bias))
        if masks:
            blocks = []
            for row in range(0, score.shape[0], ROWS):
                line = [score[row : row + ROWS, at : at + ROWS] for at in range(0, score.shape[1], ROWS)]
                for index, part in enumerate(line):
                    mask = masks.get((row // ROWS, index))
                    if mask is not None:
                        line[index] = part + mask
                blocks.append(jnp.concatenate(line, axis=1))
            score = jnp.concatenate(blocks, axis=0)
        top = jnp.max(score, axis=1, keepdims=True)
        weight = jnp.exp(score - top).astype(BF16)
        both = dot(weight, jnp.where(side, values, jnp.ones_like(values)))
        other = pltpu.roll(both, LANES // len(sides), 1)
        top = jnp.broadcast_to(top, both.shape)
        if peak is None:
            peak, mixed, total = top, both, other
        else:
            peak, mixed, total = (
                jnp.where(side, new, old) for new, old in ((top, peak), (both, mixed), (other, total))
            )
    return peak, mixed, total


def merge(first, second):
    peak = jnp.maximum(first[0], second[0])
    left, right = jnp.exp(first[0] - peak), jnp.exp(second[0] - peak)
    mixed = first[1] * left + second[1] * right
    total = first[2] * left + second[2] * right
    return mixed / total


def tile_at(tile):
    return pl.ds(pl.multiple_of(tile * LANES, LANES), LANES)


def row_step(nodes, keys):
    return nodes if nodes * keys <= SCORES else math.gcd(nodes, ROWS)


def project_observations(chunks, w_kv, keys, values, bias):
    feat = w_kv.shape[0]
    base = 0
    for chunk in chunks:
        size = chunk.shape[0]
        block = chunk[...].astype(F32)
        live = block[:, :1] < jnp.inf
        normed = rms_norm(jnp.where(live, block, 0.0))
        part = slice(base, base + size)
        keys[part] = dot(normed, w_kv[:, :feat]).astype(BF16)
        values[part] = dot(normed, w_kv[:, feat:]).astype(BF16)
        bias[part] = jnp.broadcast_to(jnp.where(live, 0.0, MASKED), (size, LANES)).astype(BF16)
        base += size


def cross_head_kernel(width, query, w_kv, *refs):
    chunks, (peak, mixed, total, keys, values, bias) = refs[:-6], refs[-6:]
    nodes, feat = query.shape
    project_observations(chunks, w_kv, keys, values, bias)
    sides = head_sides(width)
    step = row_step(nodes, keys.shape[0])

    @pl.loop(0, feat // LANES)
    def _(tile):
        at = tile_at(tile)
        for start in range(0, nodes, step):
            part = slice(start, start + step)
            peak[part, at], mixed[part, at], total[part, at] = softmax_part(
                query[part, at], keys[:, at], values[:, at], sides, bias[...]
            )


def cross_tail_kernel(
    width, latent, query, w_kv, w_out, peak, mixed, total, chunk, out, first, last, keys, values, bias, ctx
):
    nodes, feat = query.shape
    project_observations([chunk], w_kv, keys, values, bias)
    sides = head_sides(width)
    step = row_step(nodes, keys.shape[0])

    @pl.loop(0, feat // LANES)
    def _(tile):
        at = tile_at(tile)
        for start in range(0, nodes, step):
            part = slice(start, start + step)
            rest = softmax_part(query[part, at], keys[:, at], values[:, at], sides, bias[...])
            ctx[part, at] = merge((peak[part, at], mixed[part, at], total[part, at]), rest).astype(BF16)

    after = (latent[...].astype(F32) + dot(ctx[...], w_out[...])).astype(BF16)
    out[...] = after
    first[...] = after[: first.shape[0]]
    last[...] = after[nodes - last.shape[0] :]


def cross_attention(latent, queries, rows, w_kv, w_out, half):
    nodes, feat = latent.shape
    width = feat // HEADS
    chunks, last = rows[:-1], rows[-1]
    size = sum(chunk.shape[0] for chunk in chunks)
    state = pl.pallas_call(
        functools.partial(cross_head_kernel, width),
        out_shape=[jax.ShapeDtypeStruct((nodes, feat), F32)] * 3,
        in_specs=[vmem()] * (2 + len(chunks)),
        out_specs=[vmem()] * 3,
        scratch_shapes=[
            pltpu.VMEM((size, feat), BF16),
            pltpu.VMEM((size, feat), BF16),
            pltpu.VMEM((size, LANES), BF16),
        ],
        compiler_params=params(min(60, 14 + 16 * size // 1024)),
        cost_estimate=pl.CostEstimate(flops=16_000_000_000, bytes_accessed=12 << 20, transcendentals=0),
        name="cross_head",
    )(queries, w_kv, *chunks)
    size = last.shape[0]
    return pl.pallas_call(
        functools.partial(cross_tail_kernel, width),
        out_shape=[jax.ShapeDtypeStruct((count, feat), BF16) for count in (nodes, half, half)],
        in_specs=[vmem()] * 8,
        out_specs=[vmem()] * 3,
        scratch_shapes=[
            pltpu.VMEM((size, feat), BF16),
            pltpu.VMEM((size, feat), BF16),
            pltpu.VMEM((size, LANES), BF16),
            pltpu.VMEM((nodes, feat), BF16),
        ],
        compiler_params=params(20),
        cost_estimate=pl.CostEstimate(flops=7_000_000_000, bytes_accessed=12 << 20, transcendentals=0),
        name="cross_tail",
    )(latent, queries, w_kv, w_out, *state, last)


def edge_masks():
    row = lax.broadcasted_iota(jnp.int32, (ROWS, ROWS), 0)
    col = lax.broadcasted_iota(jnp.int32, (ROWS, ROWS), 1)
    return jnp.where(col >= row, 0.0, MASKED), jnp.where(col <= row, 0.0, MASKED)


def window_local_kernel(width, half, own, w_qkv, query, peak, mixed, total, keys, values):
    nodes, feat = own.shape
    normed = rms_norm(own[...])
    scale = jnp.asarray(1.0 / math.sqrt(width), BF16)
    query[...] = dot(normed, w_qkv[:, :feat]).astype(BF16) * scale
    keys[...] = dot(normed, w_qkv[:, feat : 2 * feat]).astype(BF16)
    values[...] = dot(normed, w_qkv[:, 2 * feat :]).astype(BF16)
    sides = head_sides(width)
    reach = half // ROWS
    count = nodes // ROWS
    before, after = edge_masks()

    masks = {}
    for block in range(count):
        for other in range(count):
            if other - block == -reach:
                masks[block, other] = before
            elif other - block == reach:
                masks[block, other] = after
            elif abs(other - block) > reach:
                masks[block, other] = MASKED

    @pl.loop(0, feat // LANES)
    def _(tile):
        at = tile_at(tile)
        peak[:, at], mixed[:, at], total[:, at] = softmax_part(
            query[:, at], keys[:, at], values[:, at], sides, masks=masks
        )


def window_halo_kernel(
    width, edge, own, query, peak, mixed, total, low, high, w_qkv, w_out, out, keys, values, bias, ctx
):
    nodes, feat = own.shape
    half = low.shape[0]
    for base, rows, gate in ((0, low, 0), (half, high, 1)):
        normed = rms_norm(rows[...])
        part = slice(base, base + half)
        keys[part] = dot(normed, w_qkv[:, feat : 2 * feat]).astype(BF16)
        values[part] = dot(normed, w_qkv[:, 2 * feat :]).astype(BF16)
        bias[part] = jnp.full((half, LANES), edge[gate], F32).astype(BF16)
    sides = head_sides(width)
    reach = half // ROWS
    count = nodes // ROWS
    before, after = edge_masks()

    @pl.loop(0, feat // LANES)
    def _(tile):
        at = tile_at(tile)
        for block in range(count):
            part = slice(block * ROWS, (block + 1) * ROWS)
            first, stop = min(block, reach), max(reach, block + 2 * reach - count + 1)
            state = (peak[part, at], mixed[part, at], total[part, at])
            if stop > first:
                masks = {}
                if block < reach:
                    masks[0, 0] = before
                if block + 2 * reach - count >= reach:
                    masks[0, stop - first - 1] = after
                span = slice(first * ROWS, stop * ROWS)
                other = softmax_part(query[part, at], keys[span, at], values[span, at], sides, bias[span], masks)
                ctx[part, at] = merge(state, other).astype(BF16)
            else:
                ctx[part, at] = (state[1] / state[2]).astype(BF16)

    out[...] = (own[...].astype(F32) + dot(ctx[...], w_out[...])).astype(BF16)


def window_local(own, half, w_qkv):
    nodes, feat = own.shape
    return pl.pallas_call(
        functools.partial(window_local_kernel, feat // HEADS, half),
        out_shape=[jax.ShapeDtypeStruct((nodes, feat), BF16)] + [jax.ShapeDtypeStruct((nodes, feat), F32)] * 3,
        in_specs=[vmem()] * 2,
        out_specs=[vmem()] * 4,
        scratch_shapes=[pltpu.VMEM((nodes, feat), BF16), pltpu.VMEM((nodes, feat), BF16)],
        compiler_params=params(24),
        cost_estimate=pl.CostEstimate(flops=15_000_000_000, bytes_accessed=12 << 20, transcendentals=0),
        name="window_local",
    )(own, w_qkv)


def window_halo(edge, own, local, low, high, w_qkv, w_out):
    nodes, feat = own.shape
    half = low.shape[0]
    return pl.pallas_call(
        functools.partial(window_halo_kernel, feat // HEADS),
        out_shape=jax.ShapeDtypeStruct((nodes, feat), BF16),
        in_specs=[pl.BlockSpec(memory_space=pltpu.SMEM)] + [vmem()] * 9,
        out_specs=vmem(),
        scratch_shapes=[
            pltpu.VMEM((2 * half, feat), BF16),
            pltpu.VMEM((2 * half, feat), BF16),
            pltpu.VMEM((2 * half, LANES), BF16),
            pltpu.VMEM((nodes, feat), BF16),
        ],
        compiler_params=params(24),
        cost_estimate=pl.CostEstimate(flops=10_000_000_000, bytes_accessed=12 << 20, transcendentals=0),
        name="window_halo",
    )(edge, own, *local, low, high, w_qkv, w_out)


def mlp_kernel(group, rows, *refs):
    pieces, (out, held, normed, total, sems) = refs[:-5], refs[-5:]
    slots = held.shape[0]
    blocks = [[]]
    filled = 0
    for piece in pieces:
        at = 0
        while at < piece.shape[0]:
            size = min(group - filled, piece.shape[0] - at)
            blocks[-1].append((piece, at, size, filled))
            at, filled = at + size, filled + size
            if filled == group:
                blocks.append([])
                filled = 0
    blocks.pop()

    def copies(index):
        slot = index % slots
        return [
            pltpu.make_async_copy(
                piece.at[pl.ds(at, size)], held.at[slot, pl.ds(filled, size)], sems.at[slot, filled]
            )
            for piece, at, size, filled in blocks[index]
        ]

    for index in range(min(slots, len(blocks))):
        for copy in copies(index):
            copy.start()
    normed[...] = rms_norm(rows[...])
    total[...] = rows[...].astype(F32)
    hidden = None
    for index in range(len(blocks) + 1):
        ready = None
        if index < len(blocks):
            for copy in copies(index):
                copy.wait()
            slot = index % slots
            ready = dot(normed[...], jnp.concatenate([held[slot, k, 0] for k in range(group)], axis=1))
        if index > 0:
            slot = (index - 1) % slots
            total[...] += dot_t(hidden, jnp.concatenate([held[slot, k, 1] for k in range(group)], axis=1))
            if index - 1 + slots < len(blocks):
                for copy in copies(index - 1 + slots):
                    copy.start()
        if ready is not None:
            hidden = jax.nn.gelu(ready, approximate=True).astype(BF16)
    out[...] = total[...].astype(BF16)


def mlp(rows, pieces):
    nodes, feat = rows.shape
    width = pieces[0].shape[-1]
    group = math.gcd(sum(piece.shape[0] for piece in pieces), max(1, 512 // width))
    return pl.pallas_call(
        functools.partial(mlp_kernel, group),
        out_shape=jax.ShapeDtypeStruct((nodes, feat), BF16),
        in_specs=[vmem()] + [hbm()] * len(pieces),
        out_specs=vmem(),
        scratch_shapes=[
            pltpu.VMEM((3, group, 2, feat, width), BF16),
            pltpu.VMEM((nodes, feat), BF16),
            pltpu.VMEM((nodes, feat), F32),
            pltpu.SemaphoreType.DMA((3, group)),
        ],
        compiler_params=params(18 + (12 * group * feat * max(width, LANES) >> 20)),
        cost_estimate=pl.CostEstimate(flops=8_000_000_000, bytes_accessed=18 << 20, transcendentals=0),
        name="mlp",
    )(rows, *pieces)


def shards(
    latent,
    observations,
    counts,
    cross_query,
    cross_kv,
    cross_out,
    self_qkv,
    self_out,
    mlp_in,
    mlp_out,
):
    everyone = ("loc", "stream")
    feat = latent.shape[1]
    width = feat // HEADS
    half = WIN // 2
    streams, places = lax.axis_size("stream"), lax.axis_size("loc")
    stream = lax.axis_index("stream")

    def rotate(value, shift):
        return lax.ppermute(value, "stream", [(i, (i + shift) % streams) for i in range(streams)])

    def pass_on(value, step):
        pairs = [(i, i + step) for i in range(1, streams - 1)]
        return lax.ppermute(value, "stream", pairs)

    def near_far(value):
        near = [rotate(value, shift) for shift in sorted({1, streams - 1} - {streams})]
        if streams == 4:
            far = [jnp.where(stream >= 2, pass_on(near[0], 1), pass_on(near[1], -1))]
        else:
            far = [rotate(value, shift) for shift in range(2, streams - 1)]
        return near, far

    def spread(piece):
        if places & (places - 1):
            return [lax.all_gather(piece, "loc", axis=0, tiled=True)]
        flip = [[(i, i ^ mask) for i in range(places)] for mask in range(places)]
        parts = [piece] + [lax.ppermute(piece, "loc", flip[mask]) for mask in range(2, places, 2)]
        return parts + [lax.ppermute(part, "loc", flip[1]) for part in parts]

    held = jnp.stack([mlp_in, mlp_out])[None]
    near, far = near_far(held)
    pieces = spread(held)
    if near:
        pieces += spread(jnp.concatenate(near))
    if far:
        pieces += spread(jnp.concatenate(far))
    slot = lax.broadcasted_iota(jnp.int32, observations.shape[:4], 3)
    marked = jnp.where((slot < counts[..., None])[..., None], observations, jnp.asarray(jnp.inf, BF16))
    moved = lax.all_to_all(marked, "loc", split_axis=2, concat_axis=1, tiled=True).reshape(-1, feat)
    near, far = near_far(moved)
    rows = [moved] + near + far
    queries = dot(rms_norm(latent), cross_query).astype(BF16) * jnp.asarray(1.0 / math.sqrt(width), BF16)
    after_cross, first, last = cross_attention(latent, queries, rows, cross_kv, cross_out, half)
    count = lax.axis_size(everyone)
    low = lax.ppermute(last, everyone, [(i, i + 1) for i in range(count - 1)])
    high = lax.ppermute(first, everyone, [(i + 1, i) for i in range(count - 1)])
    local = window_local(after_cross, half, self_qkv)
    place = lax.axis_index(everyone)
    edge = jnp.where(jnp.stack([place == 0, place == count - 1]), MASKED, 0.0).astype(F32)
    after_self = window_halo(edge, after_cross, local, low, high, self_qkv, self_out)
    return mlp(after_self, pieces)


def solution(mesh):
    return jax.shard_map(
        shards,
        mesh=mesh,
        in_specs=(
            P(("loc", "stream"), None),
            P("stream", "loc", None, None, None),
            P("stream", "loc", None),
            P(),
            P(),
            P(),
            P(),
            P(),
            P(None, ("loc", "stream")),
            P(None, ("loc", "stream")),
        ),
        out_specs=P(("loc", "stream"), None),
        check_vma=False,
    )
```

```python
import functools
import math

import jax
import jax.numpy as jnp
from jax import lax
from jax.experimental import pallas as pl
from jax.experimental.pallas import tpu as pltpu
from jax.sharding import PartitionSpec as P


HEADS = 16
WIN = 512

EPSILON = 1e-06
MASKED = -1e30
LANES = 128
ROWS = 128
SCORES = 1 << 19


F32 = jnp.float32
BF16 = jnp.bfloat16


def rms_norm(tensor):
    floats = tensor.astype(F32)
    return (floats * lax.rsqrt(jnp.mean(floats * floats, axis=-1, keepdims=True) + EPSILON)).astype(BF16)


def dot(a, b):
    return jnp.dot(a, b, preferred_element_type=F32)


def dot_t(a, b):
    return lax.dot_general(a, b, (((1,), (1,)), ((), ())), preferred_element_type=F32)


def vmem():
    return pl.BlockSpec(memory_space=pltpu.VMEM)


def hbm():
    return pl.BlockSpec(memory_space=pltpu.HBM)


def params(mib):
    return pltpu.CompilerParams(vmem_limit_bytes=mib << 20)


def head_sides(width):
    lane = lax.broadcasted_iota(jnp.int32, (1, LANES), 1)
    return [(lane >= at) & (lane < at + width) for at in range(0, LANES, width)]


def softmax_part(query, keys, values, sides, bias=None, masks=None):
    peak = mixed = total = None
    for side in sides:
        if bias is None:
            score = dot_t(query, jnp.where(side, keys, jnp.zeros_like(keys)))
        else:
            score = dot_t(jnp.where(side, query, jnp.ones_like(query)), jnp.where(side, keys, bias))
        if masks:
            blocks = []
            for row in range(0, score.shape[0], ROWS):
                line = [score[row : row + ROWS, at : at + ROWS] for at in range(0, score.shape[1], ROWS)]
                for index, part in enumerate(line):
                    mask = masks.get((row // ROWS, index))
                    if mask is not None:
                        line[index] = part + mask
                blocks.append(jnp.concatenate(line, axis=1))
            score = jnp.concatenate(blocks, axis=0)
        top = jnp.max(score, axis=1, keepdims=True)
        weight = jnp.exp(score - top).astype(BF16)
        both = dot(weight, jnp.where(side, values, jnp.ones_like(values)))
        other = pltpu.roll(both, LANES // len(sides), 1)
        top = jnp.broadcast_to(top, both.shape)
        if peak is None:
            peak, mixed, total = top, both, other
        else:
            peak, mixed, total = (
                jnp.where(side, new, old) for new, old in ((top, peak), (both, mixed), (other, total))
            )
    return peak, mixed, total


def merge(first, second):
    peak = jnp.maximum(first[0], second[0])
    left, right = jnp.exp(first[0] - peak), jnp.exp(second[0] - peak)
    mixed = first[1] * left + second[1] * right
    total = first[2] * left + second[2] * right
    return mixed / total


def tile_at(tile):
    return pl.ds(pl.multiple_of(tile * LANES, LANES), LANES)


def row_step(nodes, keys):
    return nodes if nodes * keys <= SCORES else math.gcd(nodes, ROWS)


def project_observations(chunks, w_kv, keys, values, bias):
    feat = w_kv.shape[0]
    base = 0
    for chunk in chunks:
        size = chunk.shape[0]
        block = chunk[...].astype(F32)
        live = block[:, :1] < jnp.inf
        normed = rms_norm(jnp.where(live, block, 0.0))
        part = slice(base, base + size)
        keys[part] = dot(normed, w_kv[:, :feat]).astype(BF16)
        values[part] = dot(normed, w_kv[:, feat:]).astype(BF16)
        bias[part] = jnp.broadcast_to(jnp.where(live, 0.0, MASKED), (size, LANES)).astype(BF16)
        base += size


def cross_head_kernel(width, query, w_kv, *refs):
    chunks, (peak, mixed, total, keys, values, bias) = refs[:-6], refs[-6:]
    nodes, feat = query.shape
    project_observations(chunks, w_kv, keys, values, bias)
    sides = head_sides(width)
    step = row_step(nodes, keys.shape[0])

    @pl.loop(0, feat // LANES, unroll=4)
    def _(tile):
        at = tile_at(tile)

        @pl.loop(0, nodes // step)
        def _(block):
            part = pl.ds(pl.multiple_of(block * step, step), step)
            peak[part, at], mixed[part, at], total[part, at] = softmax_part(
                query[part, at], keys[:, at], values[:, at], sides, bias[...]
            )


def cross_tail_kernel(
    width, latent, query, w_kv, w_out, peak, mixed, total, chunk, out, first, last, keys, values, bias, ctx
):
    nodes, feat = query.shape
    project_observations([chunk], w_kv, keys, values, bias)
    sides = head_sides(width)
    step = row_step(nodes, keys.shape[0])

    @pl.loop(0, feat // LANES, unroll=1)
    def _(tile):
        at = tile_at(tile)

        @pl.loop(0, nodes // step)
        def _(block):
            part = pl.ds(pl.multiple_of(block * step, step), step)
            rest = softmax_part(query[part, at], keys[:, at], values[:, at], sides, bias[...])
            ctx[part, at] = merge((peak[part, at], mixed[part, at], total[part, at]), rest).astype(BF16)

    after = (latent[...].astype(F32) + dot(ctx[...], w_out[...])).astype(BF16)
    out[...] = after
    first[...] = after[: first.shape[0]]
    last[...] = after[nodes - last.shape[0] :]


def cross_attention(latent, queries, rows, w_kv, w_out, half):
    nodes, feat = latent.shape
    width = feat // HEADS
    chunks, last = rows[:-1], rows[-1]
    size = sum(chunk.shape[0] for chunk in chunks)
    state = pl.pallas_call(
        functools.partial(cross_head_kernel, width),
        out_shape=[jax.ShapeDtypeStruct((nodes, feat), F32)] * 3,
        in_specs=[vmem()] * (2 + len(chunks)),
        out_specs=[vmem()] * 3,
        scratch_shapes=[
            pltpu.VMEM((size, feat), BF16),
            pltpu.VMEM((size, feat), BF16),
            pltpu.VMEM((size, LANES), BF16),
        ],
        compiler_params=params(min(60, 14 + 16 * size // 1024)),
        cost_estimate=pl.CostEstimate(flops=16_000_000_000, bytes_accessed=12 << 20, transcendentals=0),
        name="cross_head",
    )(queries, w_kv, *chunks)
    size = last.shape[0]
    return pl.pallas_call(
        functools.partial(cross_tail_kernel, width),
        out_shape=[jax.ShapeDtypeStruct((count, feat), BF16) for count in (nodes, half, half)],
        in_specs=[vmem()] * 8,
        out_specs=[vmem()] * 3,
        scratch_shapes=[
            pltpu.VMEM((size, feat), BF16),
            pltpu.VMEM((size, feat), BF16),
            pltpu.VMEM((size, LANES), BF16),
            pltpu.VMEM((nodes, feat), BF16),
        ],
        compiler_params=params(20),
        cost_estimate=pl.CostEstimate(flops=7_000_000_000, bytes_accessed=12 << 20, transcendentals=0),
        name="cross_tail",
    )(latent, queries, w_kv, w_out, *state, last)


def edge_masks():
    row = lax.broadcasted_iota(jnp.int32, (ROWS, ROWS), 0)
    col = lax.broadcasted_iota(jnp.int32, (ROWS, ROWS), 1)
    return jnp.where(col >= row, 0.0, MASKED), jnp.where(col <= row, 0.0, MASKED)


def window_local_kernel(width, half, own, w_qkv, query, peak, mixed, total, keys, values):
    nodes, feat = own.shape
    normed = rms_norm(own[...])
    scale = jnp.asarray(1.0 / math.sqrt(width), BF16)
    query[...] = dot(normed, w_qkv[:, :feat]).astype(BF16) * scale
    keys[...] = dot(normed, w_qkv[:, feat : 2 * feat]).astype(BF16)
    values[...] = dot(normed, w_qkv[:, 2 * feat :]).astype(BF16)
    sides = head_sides(width)
    reach = half // ROWS
    count = nodes // ROWS
    before, after = edge_masks()

    masks = {}
    for block in range(count):
        for other in range(count):
            if other - block == -reach:
                masks[block, other] = before
            elif other - block == reach:
                masks[block, other] = after
            elif abs(other - block) > reach:
                masks[block, other] = MASKED

    @pl.loop(0, feat // LANES, unroll=4)
    def _(tile):
        at = tile_at(tile)
        peak[:, at], mixed[:, at], total[:, at] = softmax_part(
            query[:, at], keys[:, at], values[:, at], sides, masks=masks
        )


def window_halo_kernel(
    width, edge, own, query, peak, mixed, total, low, high, w_qkv, w_out, out, keys, values, bias, ctx
):
    nodes, feat = own.shape
    half = low.shape[0]
    for base, rows, gate in ((0, low, 0), (half, high, 1)):
        normed = rms_norm(rows[...])
        part = slice(base, base + half)
        keys[part] = dot(normed, w_qkv[:, feat : 2 * feat]).astype(BF16)
        values[part] = dot(normed, w_qkv[:, 2 * feat :]).astype(BF16)
        bias[part] = jnp.full((half, LANES), edge[gate], F32).astype(BF16)
    sides = head_sides(width)
    reach = half // ROWS
    count = nodes // ROWS
    before, after = edge_masks()

    @pl.loop(0, feat // LANES, unroll=2)
    def _(tile):
        at = tile_at(tile)
        for block in range(count):
            part = slice(block * ROWS, (block + 1) * ROWS)
            first, stop = min(block, reach), max(reach, block + 2 * reach - count + 1)
            state = (peak[part, at], mixed[part, at], total[part, at])
            if stop > first:
                masks = {}
                if block < reach:
                    masks[0, 0] = before
                if block + 2 * reach - count >= reach:
                    masks[0, stop - first - 1] = after
                span = slice(first * ROWS, stop * ROWS)
                other = softmax_part(query[part, at], keys[span, at], values[span, at], sides, bias[span], masks)
                ctx[part, at] = merge(state, other).astype(BF16)
            else:
                ctx[part, at] = (state[1] / state[2]).astype(BF16)

    out[...] = (own[...].astype(F32) + dot(ctx[...], w_out[...])).astype(BF16)


def window_local(own, half, w_qkv):
    nodes, feat = own.shape
    return pl.pallas_call(
        functools.partial(window_local_kernel, feat // HEADS, half),
        out_shape=[jax.ShapeDtypeStruct((nodes, feat), BF16)] + [jax.ShapeDtypeStruct((nodes, feat), F32)] * 3,
        in_specs=[vmem()] * 2,
        out_specs=[vmem()] * 4,
        scratch_shapes=[pltpu.VMEM((nodes, feat), BF16), pltpu.VMEM((nodes, feat), BF16)],
        compiler_params=params(24),
        cost_estimate=pl.CostEstimate(flops=15_000_000_000, bytes_accessed=12 << 20, transcendentals=0),
        name="window_local",
    )(own, w_qkv)


def window_halo(edge, own, local, low, high, w_qkv, w_out):
    nodes, feat = own.shape
    half = low.shape[0]
    return pl.pallas_call(
        functools.partial(window_halo_kernel, feat // HEADS),
        out_shape=jax.ShapeDtypeStruct((nodes, feat), BF16),
        in_specs=[pl.BlockSpec(memory_space=pltpu.SMEM)] + [vmem()] * 9,
        out_specs=vmem(),
        scratch_shapes=[
            pltpu.VMEM((2 * half, feat), BF16),
            pltpu.VMEM((2 * half, feat), BF16),
            pltpu.VMEM((2 * half, LANES), BF16),
            pltpu.VMEM((nodes, feat), BF16),
        ],
        compiler_params=params(24),
        cost_estimate=pl.CostEstimate(flops=10_000_000_000, bytes_accessed=12 << 20, transcendentals=0),
        name="window_halo",
    )(edge, own, *local, low, high, w_qkv, w_out)


def gelu(x):
    slope = 2.0 * math.sqrt(2.0 / math.pi)
    return x * jax.nn.sigmoid(x * (slope + slope * 0.044715 * (x * x)))


def mlp_kernel(group, rows, base, *refs):
    pieces, (out, held, normed, total, sems) = refs[:-5], refs[-5:]
    slots = held.shape[0]
    blocks = [[]]
    filled = 0
    for piece in pieces:
        at = 0
        while at < piece.shape[0]:
            size = min(group - filled, piece.shape[0] - at)
            blocks[-1].append((piece, at, size, filled))
            at, filled = at + size, filled + size
            if filled == group:
                blocks.append([])
                filled = 0
    blocks.pop()

    def copies(index):
        slot = index % slots
        return [
            pltpu.make_async_copy(
                piece.at[pl.ds(at, size)], held.at[slot, pl.ds(filled, size)], sems.at[slot, filled]
            )
            for piece, at, size, filled in blocks[index]
        ]

    for index in range(min(slots, len(blocks))):
        for copy in copies(index):
            copy.start()
    normed[...] = rms_norm(rows[...])
    total[...] = base[...].astype(F32)
    hidden = None
    for index in range(len(blocks) + 1):
        ready = None
        if index < len(blocks):
            for copy in copies(index):
                copy.wait()
            slot = index % slots
            ready = dot(normed[...], jnp.concatenate([held[slot, k, 0] for k in range(group)], axis=1))
        if index > 0:
            slot = (index - 1) % slots
            total[...] += dot_t(hidden, jnp.concatenate([held[slot, k, 1] for k in range(group)], axis=1))
            if index - 1 + slots < len(blocks):
                for copy in copies(index - 1 + slots):
                    copy.start()
        if ready is not None:
            hidden = gelu(ready).astype(BF16)
    out[...] = total[...].astype(out.dtype)


def mlp(rows, base, pieces, dtype):
    nodes, feat = rows.shape
    width = pieces[0].shape[-1]
    group = math.gcd(sum(piece.shape[0] for piece in pieces), max(1, 1024 // max(width, LANES)))
    return pl.pallas_call(
        functools.partial(mlp_kernel, group),
        out_shape=jax.ShapeDtypeStruct((nodes, feat), dtype),
        in_specs=[vmem()] * 2 + [hbm()] * len(pieces),
        out_specs=vmem(),
        scratch_shapes=[
            pltpu.VMEM((3, group, 2, feat, width), BF16),
            pltpu.VMEM((nodes, feat), BF16),
            pltpu.VMEM((nodes, feat), F32),
            pltpu.SemaphoreType.DMA((3, group)),
        ],
        compiler_params=params(18 + (12 * group * feat * max(width, LANES) >> 20)),
        cost_estimate=pl.CostEstimate(flops=6_000_000_000, bytes_accessed=12 << 20, transcendentals=0),
    )(rows, base, *pieces)


def shards(
    latent,
    observations,
    counts,
    cross_query,
    cross_kv,
    cross_out,
    self_qkv,
    self_out,
    mlp_in,
    mlp_out,
):
    everyone = ("loc", "stream")
    feat = latent.shape[1]
    width = feat // HEADS
    half = WIN // 2
    streams, places = lax.axis_size("stream"), lax.axis_size("loc")
    stream = lax.axis_index("stream")

    def rotate(value, shift):
        return lax.ppermute(value, "stream", [(i, (i + shift) % streams) for i in range(streams)])

    def pass_on(value, step):
        pairs = [(i, i + step) for i in range(1, streams - 1)]
        return lax.ppermute(value, "stream", pairs)

    def near_far(value):
        near = [rotate(value, shift) for shift in sorted({1, streams - 1} - {streams})]
        if streams == 4:
            far = [jnp.where(stream >= 2, pass_on(near[0], 1), pass_on(near[1], -1))]
        else:
            far = [rotate(value, shift) for shift in range(2, streams - 1)]
        return near, far

    def spread(piece, turn):
        if places & (places - 1):
            return [lax.all_gather(piece, "loc", axis=0, tiled=True)]
        flip = [[(i, i ^ mask) for i in range(places)] for mask in range(places)]
        masks = [1 << bit for bit in range(1, places.bit_length() - 1)][::turn]
        parts = [piece]
        for mask in masks:
            for part in list(parts):
                parts.append(lax.ppermute(part, "loc", flip[mask]))
        return parts + [lax.ppermute(part, "loc", flip[1]) for part in parts]

    held = jnp.stack([mlp_in, mlp_out])[None]
    near, far = near_far(held)
    pieces = spread(held, 1)
    for index, piece in enumerate(near):
        pieces += spread(piece, 1 - 2 * (index % 2))
    late = []
    for index, piece in enumerate(far):
        late += spread(piece, 2 * (index % 2) - 1)
    slot = lax.broadcasted_iota(jnp.int32, observations.shape[:4], 3)
    marked = jnp.where((slot < counts[..., None])[..., None], observations, jnp.asarray(jnp.inf, BF16))
    moved = lax.all_to_all(marked, "loc", split_axis=2, concat_axis=1, tiled=True).reshape(-1, feat)
    near, far = near_far(moved)
    rows = [moved] + near + far
    queries = dot(rms_norm(latent), cross_query).astype(BF16) * jnp.asarray(1.0 / math.sqrt(width), BF16)
    after_cross, first, last = cross_attention(latent, queries, rows, cross_kv, cross_out, half)
    count = lax.axis_size(everyone)
    low = lax.ppermute(last, everyone, [(i, i + 1) for i in range(count - 1)])
    high = lax.ppermute(first, everyone, [(i + 1, i) for i in range(count - 1)])
    local = window_local(after_cross, half, self_qkv)
    place = lax.axis_index(everyone)
    edge = jnp.where(jnp.stack([place == 0, place == count - 1]), MASKED, 0.0).astype(F32)
    after_self = window_halo(edge, after_cross, local, low, high, self_qkv, self_out)
    if not late:
        return mlp(after_self, after_self, pieces, BF16)
    partial = mlp(after_self, after_self, pieces, F32)
    return mlp(after_self, partial, late, BF16)


def solution(mesh):
    return jax.shard_map(
        shards,
        mesh=mesh,
        in_specs=(
            P(("loc", "stream"), None),
            P("stream", "loc", None, None, None),
            P("stream", "loc", None),
            P(),
            P(),
            P(),
            P(),
            P(),
            P(None, ("loc", "stream")),
            P(None, ("loc", "stream")),
        ),
        out_specs=P(("loc", "stream"), None),
        check_vma=False,
    )
```

```python
import functools
import math

import jax
import jax.numpy as jnp
from jax import lax
from jax.experimental import pallas as pl
from jax.experimental.pallas import tpu as pltpu
from jax.sharding import PartitionSpec as P


HEADS = 16
WIN = 512

EPSILON = 1e-06
MASKED = -1e30
LANES = 128
ROWS = 128
SCORES = 1 << 19


F32 = jnp.float32
BF16 = jnp.bfloat16


def rms_norm(tensor):
    floats = tensor.astype(F32)
    return (floats * lax.rsqrt(jnp.mean(floats * floats, axis=-1, keepdims=True) + EPSILON)).astype(BF16)


def dot(a, b):
    return jnp.dot(a, b, preferred_element_type=F32)


def dot_t(a, b):
    return lax.dot_general(a, b, (((1,), (1,)), ((), ())), preferred_element_type=F32)


def vmem():
    return pl.BlockSpec(memory_space=pltpu.VMEM)


def hbm():
    return pl.BlockSpec(memory_space=pltpu.HBM)


def params(mib):
    return pltpu.CompilerParams(vmem_limit_bytes=mib << 20)


def head_sides(width):
    lane = lax.broadcasted_iota(jnp.int32, (1, LANES), 1)
    return [(lane >= at) & (lane < at + width) for at in range(0, LANES, width)]


def softmax_part(query, keys, values, sides, bias=None, masks=None):
    peak = mixed = total = None
    for side in sides:
        if bias is None:
            score = dot_t(query, jnp.where(side, keys, jnp.zeros_like(keys)))
        else:
            score = dot_t(jnp.where(side, query, jnp.ones_like(query)), jnp.where(side, keys, bias))
        if masks:
            blocks = []
            for row in range(0, score.shape[0], ROWS):
                line = [score[row : row + ROWS, at : at + ROWS] for at in range(0, score.shape[1], ROWS)]
                for index, part in enumerate(line):
                    mask = masks.get((row // ROWS, index))
                    if mask is not None:
                        line[index] = part + mask
                blocks.append(jnp.concatenate(line, axis=1))
            score = jnp.concatenate(blocks, axis=0)
        top = jnp.max(score, axis=1, keepdims=True)
        weight = jnp.exp(score - top).astype(BF16)
        both = dot(weight, jnp.where(side, values, jnp.ones_like(values)))
        other = pltpu.roll(both, LANES // len(sides), 1)
        top = jnp.broadcast_to(top, both.shape)
        if peak is None:
            peak, mixed, total = top, both, other
        else:
            peak, mixed, total = (
                jnp.where(side, new, old) for new, old in ((top, peak), (both, mixed), (other, total))
            )
    return peak, mixed, total


def combine(first, second):
    peak = jnp.maximum(first[0], second[0])
    left, right = jnp.exp(first[0] - peak), jnp.exp(second[0] - peak)
    mixed = first[1] * left + second[1] * right
    total = first[2] * left + second[2] * right
    return peak, mixed, total


def merge(first, second):
    _, mixed, total = combine(first, second)
    return mixed / total


def tile_at(tile):
    return pl.ds(pl.multiple_of(tile * LANES, LANES), LANES)


def row_step(nodes, keys):
    return nodes if nodes * keys <= SCORES else math.gcd(nodes, ROWS)


def project_observations(chunks, w_kv, keys, values, bias):
    feat = w_kv.shape[0]
    base = 0
    for chunk in chunks:
        size = chunk.shape[0]
        block = chunk[...].astype(F32)
        live = block[:, :1] < jnp.inf
        normed = rms_norm(jnp.where(live, block, 0.0))
        part = slice(base, base + size)
        keys[part] = dot(normed, w_kv[:, :feat]).astype(BF16)
        values[part] = dot(normed, w_kv[:, feat:]).astype(BF16)
        bias[part] = jnp.broadcast_to(jnp.where(live, 0.0, MASKED), (size, LANES)).astype(BF16)
        base += size


def cross_head_kernel(width, count, query, w_kv, *refs):
    chunks, known, (peak, mixed, total, keys, values, bias) = refs[:count], refs[count:-6], refs[-6:]
    nodes, feat = query.shape
    project_observations(chunks, w_kv, keys, values, bias)
    sides = head_sides(width)
    step = row_step(nodes, keys.shape[0])

    @pl.loop(0, feat // LANES, unroll=4)
    def _(tile):
        at = tile_at(tile)

        @pl.loop(0, nodes // step)
        def _(block):
            part = pl.ds(pl.multiple_of(block * step, step), step)
            state = softmax_part(query[part, at], keys[:, at], values[:, at], sides, bias[...])
            if known:
                state = combine([ref[part, at] for ref in known], state)
            peak[part, at], mixed[part, at], total[part, at] = state


def cross_tail_kernel(
    width, latent, query, w_kv, w_out, peak, mixed, total, chunk, out, first, last, keys, values, bias, ctx
):
    nodes, feat = query.shape
    project_observations([chunk], w_kv, keys, values, bias)
    sides = head_sides(width)
    step = row_step(nodes, keys.shape[0])

    @pl.loop(0, feat // LANES, unroll=1)
    def _(tile):
        at = tile_at(tile)

        @pl.loop(0, nodes // step)
        def _(block):
            part = pl.ds(pl.multiple_of(block * step, step), step)
            rest = softmax_part(query[part, at], keys[:, at], values[:, at], sides, bias[...])
            ctx[part, at] = merge((peak[part, at], mixed[part, at], total[part, at]), rest).astype(BF16)

    after = (latent[...].astype(F32) + dot(ctx[...], w_out[...])).astype(BF16)
    out[...] = after
    first[...] = after[: first.shape[0]]
    last[...] = after[nodes - last.shape[0] :]


def cross_head(queries, w_kv, chunks, known):
    nodes, feat = queries.shape
    size = sum(chunk.shape[0] for chunk in chunks)
    return pl.pallas_call(
        functools.partial(cross_head_kernel, feat // HEADS, len(chunks)),
        out_shape=[jax.ShapeDtypeStruct((nodes, feat), F32)] * 3,
        in_specs=[vmem()] * (2 + len(chunks) + len(known)),
        out_specs=[vmem()] * 3,
        scratch_shapes=[
            pltpu.VMEM((size, feat), BF16),
            pltpu.VMEM((size, feat), BF16),
            pltpu.VMEM((size, LANES), BF16),
        ],
        compiler_params=params(min(60, 16 + 16 * size // 1024)),
        cost_estimate=pl.CostEstimate(flops=16_000_000 * size, bytes_accessed=12 << 20, transcendentals=0),
    )(queries, w_kv, *chunks, *known)


def cross_attention(latent, queries, rows, w_kv, w_out, half):
    nodes, feat = latent.shape
    width = feat // HEADS
    first, *chunks, last = rows
    state = cross_head(queries, w_kv, [first], ())
    if chunks:
        state = cross_head(queries, w_kv, chunks, state)
    size = last.shape[0]
    return pl.pallas_call(
        functools.partial(cross_tail_kernel, width),
        out_shape=[jax.ShapeDtypeStruct((count, feat), BF16) for count in (nodes, half, half)],
        in_specs=[vmem()] * 8,
        out_specs=[vmem()] * 3,
        scratch_shapes=[
            pltpu.VMEM((size, feat), BF16),
            pltpu.VMEM((size, feat), BF16),
            pltpu.VMEM((size, LANES), BF16),
            pltpu.VMEM((nodes, feat), BF16),
        ],
        compiler_params=params(20),
        cost_estimate=pl.CostEstimate(flops=7_000_000_000, bytes_accessed=12 << 20, transcendentals=0),
        name="cross_tail",
    )(latent, queries, w_kv, w_out, *state, last)


def edge_masks():
    row = lax.broadcasted_iota(jnp.int32, (ROWS, ROWS), 0)
    col = lax.broadcasted_iota(jnp.int32, (ROWS, ROWS), 1)
    return jnp.where(col >= row, 0.0, MASKED), jnp.where(col <= row, 0.0, MASKED)


def window_local_kernel(width, half, own, w_qkv, query, peak, mixed, total, keys, values):
    nodes, feat = own.shape
    normed = rms_norm(own[...])
    scale = jnp.asarray(1.0 / math.sqrt(width), BF16)
    query[...] = dot(normed, w_qkv[:, :feat]).astype(BF16) * scale
    keys[...] = dot(normed, w_qkv[:, feat : 2 * feat]).astype(BF16)
    values[...] = dot(normed, w_qkv[:, 2 * feat :]).astype(BF16)
    sides = head_sides(width)
    reach = half // ROWS
    count = nodes // ROWS
    before, after = edge_masks()

    masks = {}
    for block in range(count):
        for other in range(count):
            if other - block == -reach:
                masks[block, other] = before
            elif other - block == reach:
                masks[block, other] = after
            elif abs(other - block) > reach:
                masks[block, other] = MASKED

    @pl.loop(0, feat // LANES, unroll=4)
    def _(tile):
        at = tile_at(tile)
        peak[:, at], mixed[:, at], total[:, at] = softmax_part(
            query[:, at], keys[:, at], values[:, at], sides, masks=masks
        )


def window_halo_kernel(
    width, edge, own, query, peak, mixed, total, low, high, w_qkv, w_out, out, keys, values, bias, ctx
):
    nodes, feat = own.shape
    half = low.shape[0]
    for base, rows, gate in ((0, low, 0), (half, high, 1)):
        normed = rms_norm(rows[...])
        part = slice(base, base + half)
        keys[part] = dot(normed, w_qkv[:, feat : 2 * feat]).astype(BF16)
        values[part] = dot(normed, w_qkv[:, 2 * feat :]).astype(BF16)
        bias[part] = jnp.full((half, LANES), edge[gate], F32).astype(BF16)
    sides = head_sides(width)
    reach = half // ROWS
    count = nodes // ROWS
    before, after = edge_masks()

    @pl.loop(0, feat // LANES, unroll=2)
    def _(tile):
        at = tile_at(tile)
        for block in range(count):
            part = slice(block * ROWS, (block + 1) * ROWS)
            first, stop = min(block, reach), max(reach, block + 2 * reach - count + 1)
            state = (peak[part, at], mixed[part, at], total[part, at])
            if stop > first:
                masks = {}
                if block < reach:
                    masks[0, 0] = before
                if block + 2 * reach - count >= reach:
                    masks[0, stop - first - 1] = after
                span = slice(first * ROWS, stop * ROWS)
                other = softmax_part(query[part, at], keys[span, at], values[span, at], sides, bias[span], masks)
                ctx[part, at] = merge(state, other).astype(BF16)
            else:
                ctx[part, at] = (state[1] / state[2]).astype(BF16)

    out[...] = (own[...].astype(F32) + dot(ctx[...], w_out[...])).astype(BF16)


def window_local(own, half, w_qkv):
    nodes, feat = own.shape
    return pl.pallas_call(
        functools.partial(window_local_kernel, feat // HEADS, half),
        out_shape=[jax.ShapeDtypeStruct((nodes, feat), BF16)] + [jax.ShapeDtypeStruct((nodes, feat), F32)] * 3,
        in_specs=[vmem()] * 2,
        out_specs=[vmem()] * 4,
        scratch_shapes=[pltpu.VMEM((nodes, feat), BF16), pltpu.VMEM((nodes, feat), BF16)],
        compiler_params=params(24),
        cost_estimate=pl.CostEstimate(flops=15_000_000_000, bytes_accessed=12 << 20, transcendentals=0),
        name="window_local",
    )(own, w_qkv)


def window_halo(edge, own, local, low, high, w_qkv, w_out):
    nodes, feat = own.shape
    half = low.shape[0]
    return pl.pallas_call(
        functools.partial(window_halo_kernel, feat // HEADS),
        out_shape=jax.ShapeDtypeStruct((nodes, feat), BF16),
        in_specs=[pl.BlockSpec(memory_space=pltpu.SMEM)] + [vmem()] * 9,
        out_specs=vmem(),
        scratch_shapes=[
            pltpu.VMEM((2 * half, feat), BF16),
            pltpu.VMEM((2 * half, feat), BF16),
            pltpu.VMEM((2 * half, LANES), BF16),
            pltpu.VMEM((nodes, feat), BF16),
        ],
        compiler_params=params(24),
        cost_estimate=pl.CostEstimate(flops=10_000_000_000, bytes_accessed=12 << 20, transcendentals=0),
        name="window_halo",
    )(edge, own, *local, low, high, w_qkv, w_out)


def gelu(x):
    slope = 2.0 * math.sqrt(2.0 / math.pi)
    return x * jax.nn.sigmoid(x * (slope + slope * 0.044715 * (x * x)))


def mlp_kernel(group, rows, base, *refs):
    pieces, (out, held, normed, total, sems) = refs[:-5], refs[-5:]
    slots = held.shape[0]
    blocks = [[]]
    filled = 0
    for piece in pieces:
        at = 0
        while at < piece.shape[0]:
            size = min(group - filled, piece.shape[0] - at)
            blocks[-1].append((piece, at, size, filled))
            at, filled = at + size, filled + size
            if filled == group:
                blocks.append([])
                filled = 0
    blocks.pop()

    def copies(index):
        slot = index % slots
        return [
            pltpu.make_async_copy(
                piece.at[pl.ds(at, size)], held.at[slot, pl.ds(filled, size)], sems.at[slot, filled]
            )
            for piece, at, size, filled in blocks[index]
        ]

    for index in range(min(slots, len(blocks))):
        for copy in copies(index):
            copy.start()
    normed[...] = rms_norm(rows[...])
    total[...] = base[...].astype(F32)
    hidden = None
    for index in range(len(blocks) + 1):
        ready = None
        if index < len(blocks):
            for copy in copies(index):
                copy.wait()
            slot = index % slots
            ready = dot(normed[...], jnp.concatenate([held[slot, k, 0] for k in range(group)], axis=1))
        if index > 0:
            slot = (index - 1) % slots
            total[...] += dot_t(hidden, jnp.concatenate([held[slot, k, 1] for k in range(group)], axis=1))
            if index - 1 + slots < len(blocks):
                for copy in copies(index - 1 + slots):
                    copy.start()
        if ready is not None:
            hidden = gelu(ready).astype(BF16)
    out[...] = total[...].astype(out.dtype)


def mlp(rows, base, pieces, dtype):
    nodes, feat = rows.shape
    width = pieces[0].shape[-1]
    group = math.gcd(sum(piece.shape[0] for piece in pieces), max(1, 1024 // max(width, LANES)))
    return pl.pallas_call(
        functools.partial(mlp_kernel, group),
        out_shape=jax.ShapeDtypeStruct((nodes, feat), dtype),
        in_specs=[vmem()] * 2 + [hbm()] * len(pieces),
        out_specs=vmem(),
        scratch_shapes=[
            pltpu.VMEM((3, group, 2, feat, width), BF16),
            pltpu.VMEM((nodes, feat), BF16),
            pltpu.VMEM((nodes, feat), F32),
            pltpu.SemaphoreType.DMA((3, group)),
        ],
        compiler_params=params(18 + (12 * group * feat * max(width, LANES) >> 20)),
        cost_estimate=pl.CostEstimate(flops=6_000_000_000, bytes_accessed=12 << 20, transcendentals=0),
    )(rows, base, *pieces)


def shards(
    latent,
    observations,
    counts,
    cross_query,
    cross_kv,
    cross_out,
    self_qkv,
    self_out,
    mlp_in,
    mlp_out,
):
    everyone = ("loc", "stream")
    feat = latent.shape[1]
    width = feat // HEADS
    half = WIN // 2
    streams, places = lax.axis_size("stream"), lax.axis_size("loc")
    stream = lax.axis_index("stream")

    def rotate(value, shift):
        return lax.ppermute(value, "stream", [(i, (i + shift) % streams) for i in range(streams)])

    def pass_on(value, step):
        pairs = [(i, i + step) for i in range(1, streams - 1)]
        return lax.ppermute(value, "stream", pairs)

    def near_far(value):
        near = [rotate(value, shift) for shift in sorted({1, streams - 1} - {streams})]
        if streams == 4:
            far = [jnp.where(stream >= 2, pass_on(near[0], 1), pass_on(near[1], -1))]
        else:
            far = [rotate(value, shift) for shift in range(2, streams - 1)]
        return near, far

    def spread(piece, turn):
        if places & (places - 1):
            return [lax.all_gather(piece, "loc", axis=0, tiled=True)]
        flip = [[(i, i ^ mask) for i in range(places)] for mask in range(places)]
        masks = [1 << bit for bit in range(1, places.bit_length() - 1)][::turn]
        parts = [piece]
        for mask in masks:
            for part in list(parts):
                parts.append(lax.ppermute(part, "loc", flip[mask]))
        return parts + [lax.ppermute(part, "loc", flip[1]) for part in parts]

    held = jnp.stack([mlp_in, mlp_out])[None]
    near, far = near_far(held)
    pieces = spread(held, 1)
    for index, piece in enumerate(near):
        pieces += spread(piece, 1 - 2 * (index % 2))
    late = []
    for index, piece in enumerate(far):
        late += spread(piece, 2 * (index % 2) - 1)
    slot = lax.broadcasted_iota(jnp.int32, observations.shape[:4], 3)
    marked = jnp.where((slot < counts[..., None])[..., None], observations, jnp.asarray(jnp.inf, BF16))
    moved = lax.all_to_all(marked, "loc", split_axis=2, concat_axis=1, tiled=True).reshape(-1, feat)
    near, far = near_far(moved)
    rows = [moved] + near + far
    queries = dot(rms_norm(latent), cross_query).astype(BF16) * jnp.asarray(1.0 / math.sqrt(width), BF16)
    after_cross, first, last = cross_attention(latent, queries, rows, cross_kv, cross_out, half)
    count = lax.axis_size(everyone)
    low = lax.ppermute(last, everyone, [(i, i + 1) for i in range(count - 1)])
    high = lax.ppermute(first, everyone, [(i + 1, i) for i in range(count - 1)])
    local = window_local(after_cross, half, self_qkv)
    place = lax.axis_index(everyone)
    edge = jnp.where(jnp.stack([place == 0, place == count - 1]), MASKED, 0.0).astype(F32)
    after_self = window_halo(edge, after_cross, local, low, high, self_qkv, self_out)
    if not late:
        return mlp(after_self, after_self, pieces, BF16)
    partial = mlp(after_self, after_self, pieces, F32)
    return mlp(after_self, partial, late, BF16)


def solution(mesh):
    return jax.shard_map(
        shards,
        mesh=mesh,
        in_specs=(
            P(("loc", "stream"), None),
            P("stream", "loc", None, None, None),
            P("stream", "loc", None),
            P(),
            P(),
            P(),
            P(),
            P(),
            P(None, ("loc", "stream")),
            P(None, ("loc", "stream")),
        ),
        out_specs=P(("loc", "stream"), None),
        check_vma=False,
    )
```
